32 devices in a mesh: band: 8 (over y, x, core), ga: 4 (over z).
Axes of the slice: x: 2, y: 2, z: 4, core: 2. Of those that a mesh axis runs over, the one named last changes fastest.
Arguments:
- wave_coef: bfloat16 [4096, 16384], P('band', 'ga'), may hold values from -0.046875 to 0.046875
- projector: bfloat16 [32, 27, 16384], P('band', None, 'ga'), may hold values from -6 to 6
- occupation: float32 [4096], P('band'), may hold values from 0.25 to 4
- species: int32 [32], replicated, may hold values from 0 to 3
- layer_in: float32 [4, 729, 100], replicated, may hold values from -1.25 to 1.25
- bias_in: float32 [4, 100], replicated, may hold values from -3 to 3
- layer_out: float32 [4, 100], replicated, may hold values from -0.625 to 0.625
Outputs:
- corrected: bfloat16 [4096, 16384], P('band', 'ga')
The draws below stay inside these ranges and needn't reach their ends.
All inputs are finite; a program needn't handle non-finite values.
Results may differ from the reference program's by a relative error of at most 0.0049.
Values may be sent and summed in bfloat16 or wider, within the bound.
A program may use at most 128 MiB of HBM per device.

```python
import math
import jax
import jax.numpy as jnp
from jax import lax

K = 27
HID = 100
SPECIES = 4
NB = 4096
NG = 16384
ATOMS = 32


def plant(entries, own_key, smallest, top_value):
    place = [jax.random.randint(jax.random.fold_in(own_key, axis), (), 0, length) for axis, length in enumerate(entries.shape)]
    main_axis = entries.shape.index(max(entries.shape))
    beside = place[:main_axis] + [(place[main_axis] + 1) % entries.shape[main_axis]] + place[main_axis + 1:]
    return entries.at[tuple(place)].set(smallest).at[tuple(beside)].set(top_value)


def steps_of(stream_key, dims, split, low, high):
    level = 1.0
    for axis_at, blocks in split:
        draws = jax.random.uniform(jax.random.fold_in(jax.random.fold_in(stream_key, 6), axis_at), (blocks,), jnp.float32, low / len(split), high / len(split))
        level = level * jnp.repeat(jnp.exp(draws), dims[axis_at] // blocks).reshape((-1,) + (1,) * (len(dims) - 1 - axis_at))
    return level


def centred(rng, extent, scale, bound, cuts=(), held_as=jnp.bfloat16):
    gain = steps_of(rng, extent, cuts, -0.22, 0.18) if cuts else 1.0
    values = jax.random.normal(rng, extent, jnp.float32) * scale * gain
    return jnp.minimum(jnp.maximum(values, -bound), bound).astype(held_as)


def setup_inputs(seed: int = 0) -> dict:
    seeds = jax.random.split(jax.random.key(seed), 8)
    return {
        "wave_coef": centred(seeds[0], (NB, NG), NG ** -0.5, 0.046875, ((0, 8), (1, 4))),
        "projector": centred(seeds[1], (ATOMS, K, NG), 1.0, 6.0, ((0, 8), (2, 4))),
        "occupation": jnp.clip(jnp.exp(math.log(4.0) - 2.7725887 * jax.random.uniform(seeds[2], (NB,), jnp.float32) ** steps_of(seeds[2], (NB,), ((0, 8),), -0.2, 0.2)), 0.25, 4.0),
        "species": plant(jax.random.randint(seeds[3], (ATOMS,), 0, SPECIES), jax.random.fold_in(seeds[3], 1), 0, SPECIES - 1).astype(jnp.int32),
        "layer_in": centred(seeds[4], (SPECIES, K * K, HID), K ** -0.5, 1.25, (), jnp.float32),
        "bias_in": centred(seeds[5], (SPECIES, HID), 0.5, 3.0, (), jnp.float32),
        "layer_out": centred(seeds[6], (SPECIES, HID), HID ** -0.5, 0.625, (), jnp.float32),
    }


def reference(wave_coef, projector, occupation, species, layer_in, bias_in, layer_out):
    flattened = projector.reshape(ATOMS * K, NG)
    coefficient = lax.dot_general(wave_coef, flattened, (((1,), (1,)), ((), ())), preferred_element_type=jnp.float32)
    coefficient = coefficient.reshape(NB, ATOMS, K)
    density = jnp.einsum('n,nak,nal->akl', occupation, coefficient, coefficient, precision=lax.Precision.HIGHEST) / NB
    onehot = (species[:, None] == jnp.arange(SPECIES, dtype=jnp.int32)[None, :]).astype(jnp.float32)
    weight_atom = jnp.einsum('as,sfh->afh', onehot, layer_in, precision=lax.Precision.HIGHEST)
    bias_atom = jnp.dot(onehot, bias_in, precision=lax.Precision.HIGHEST)
    out_atom = jnp.dot(onehot, layer_out, precision=lax.Precision.HIGHEST)
    preact = jnp.einsum('af,afh->ah', density.reshape(ATOMS, K * K), weight_atom, precision=lax.Precision.HIGHEST) + bias_atom
    activation = jnp.tanh(preact)
    slopes = out_atom * (1.0 - activation * activation)
    gradient = jnp.einsum('afh,ah->af', weight_atom, slopes, precision=lax.Precision.HIGHEST).reshape(ATOMS, K, K)
    symmetric = gradient + jnp.swapaxes(gradient, 1, 2)
    factor = 1.0 / jnp.sqrt(jnp.float32(ATOMS * K))
    applied = (jnp.einsum('akl,nal->nak', symmetric, coefficient, precision=lax.Precision.HIGHEST) * factor).astype(jnp.bfloat16)
    corrected = jnp.dot(applied.reshape(NB, ATOMS * K), flattened, preferred_element_type=jnp.float32)
    return corrected.astype(jnp.bfloat16)
```

```python
import functools

import jax
import jax.numpy as jnp
from jax import lax
from jax.experimental import pallas as pl
from jax.experimental.pallas import tpu as pltpu
from jax.sharding import PartitionSpec as P

MESH = pl.DeviceIdType.MESH
F32 = jnp.float32
BF16 = jnp.bfloat16
PIECES = 4
LPAD = 32


def split(value):
    high = value.astype(BF16)
    return high, (value - high.astype(F32)).astype(BF16)


def dot(a, b, contract):
    return lax.dot_general(a, b, ((contract[:1], contract[1:]), ((), ())), preferred_element_type=F32)


def kernel(dims, wave_hbm, proj_hbm, occ_ref, species_ref, layer_hbm, bias_ref, out_ref,
           app_ref, whole_ref,
           gp, wave, pacc, part, prcv, cbf, layer, wpad, whi, wlo, mask, fold, bias_pad, lout_pad,
           dsend, drcv, dwide, dts, dflat, gs, scs, scr, appo, tmp,
           load_sem, keep_sem, xs, xr, ss, sr, zs, zr, cs, cr, ds_, dr, gs_s, gs_r):
    nb, ga, apd, K, nspec, hid = dims
    npair = nb // 2
    unit = 2 * apd
    qa = unit // ga
    q = qa * K
    qp = part.shape[2]
    rows = npair * qp
    blk = gp.shape[2]
    bands, gloc = wave.shape
    owned = npair * qa
    shift = qp.bit_length() - 1
    plane = npair == 4
    b = lax.axis_index("band")
    z = lax.axis_index("ga")
    chip, core = b // 2, b % 2

    def peer_chip(d):
        if plane:
            x, y = chip % 2, chip // 2
            x = 1 - x if d % 2 else x
            y = 1 - y if d // 2 else y
            return y * 2 + x
        return lax.rem(chip + d, npair)

    def from_chip(d):
        if plane:
            return peer_chip(d)
        return lax.rem(chip + npair - d, npair)

    sibling = chip * 2 + 1 - core
    width = gloc // PIECES

    def cols(i):
        return pl.ds(i * width, width)

    loads = [
        pltpu.make_async_copy(proj_hbm, gp.at[chip, core], load_sem.at[0]),
        pltpu.make_async_copy(wave_hbm, wave, load_sem.at[1]),
        pltpu.make_async_copy(layer_hbm, layer, load_sem.at[2]),
    ]
    for c in loads:
        c.start()

    barrier = pltpu.get_barrier_semaphore()
    for d in range(1, nb):
        pl.semaphore_signal(barrier, inc=1, device_id=(lax.rem(b + d, nb), z), device_id_type=MESH)
    for d in range(1, ga):
        pl.semaphore_signal(barrier, inc=1, device_id=(b, lax.rem(z + d, ga)), device_id_type=MESH)
    pl.semaphore_wait(barrier, nb + ga - 2)

    sends = []

    def remote(src, dst, send_sem, recv_sem, where):
        copy = pltpu.make_async_remote_copy(src_ref=src, dst_ref=dst, send_sem=send_sem, recv_sem=recv_sem,
                                            device_id=where, device_id_type=MESH)
        return copy

    def chip_copy(d, i, block_chip, target_chip, send_d):
        view = gp.at[block_chip, core, :, cols(i)]
        return remote(view, view, xs.at[send_d, i], xr.at[d, i], (target_chip * 2 + core, z))

    def sib_copy(d, i, block_chip):
        view = gp.at[block_chip, core, :, cols(i)]
        return remote(view, view, ss.at[d, i], sr.at[d, i], (sibling, z))

    def go(copy):
        copy.start()
        sends.append(copy)

    half = PIECES // 2
    order1 = list(range(PIECES))
    order2 = order1[half:] + order1[:half]
    loads[0].wait()
    for n in range(PIECES):
        if plane:
            go(chip_copy(1, order1[n], chip, peer_chip(1), 1))
            go(chip_copy(2, order2[n], chip, peer_chip(2), 2))
        else:
            for d in range(1, npair):
                go(chip_copy(d, n, chip, peer_chip(d), d))
    for n in range(PIECES):
        go(sib_copy(0, n, chip))

    wpad[...] = jnp.zeros_like(wpad)
    bias_pad[...] = jnp.zeros_like(bias_pad)
    lout_pad[...] = jnp.zeros_like(lout_pad)
    dwide[...] = jnp.zeros_like(dwide)
    gs[...] = jnp.zeros_like(gs)
    dflat[...] = jnp.zeros_like(dflat)
    tmp[...] = jnp.zeros_like(tmp)

    def place(i, axis_shape, axis):
        idx = lax.broadcasted_iota(jnp.int32, axis_shape, axis)
        pair = idx >> shift
        w = idx - (pair << shift)
        j = jnp.zeros_like(w)
        for t in range(1, qa):
            j = j + (w >= t * K).astype(jnp.int32)
        return pair * qa + j, w - j * K, w < q

    ar, _, vr = place(0, (rows, rows), 0)
    ac, _, vc = place(0, (rows, rows), 1)
    mask[...] = jnp.where((ar == ac) & vr & vc, 1.0, 0.0).astype(F32)
    _, kc, vk = place(0, (LPAD, rows), 1)
    lrow = lax.broadcasted_iota(jnp.int32, (LPAD, rows), 0)
    fold[...] = jnp.where((lrow == kc) & vk, 1.0, 0.0).astype(F32).astype(BF16)

    for s in range(nspec):
        bias_pad[0:1, s * 128:s * 128 + hid] = bias_ref[s:s + 1, :]
        lout_pad[0:1, s * 128:s * 128 + hid] = out_ref[s:s + 1, :]
    loads[2].wait()
    for s in range(nspec):
        for k in range(K):
            wpad[k * LPAD:k * LPAD + K, s * 128:s * 128 + hid] = layer[s, k * K:(k + 1) * K, :]
    high, low = split(wpad[...])
    whi[...] = high
    wlo[...] = low
    loads[1].wait()

    keeps = []
    ntile = 256 if bands % 256 == 0 else bands

    def project(stage, p):
        for c in range(2):
            k = pltpu.make_async_copy(gp.at[p, c], whole_ref.at[pl.ds(pl.multiple_of((p * 2 + c) * blk, blk), blk)],
                                      keep_sem.at[stage, c])
            k.start()
            keeps.append(k)
        lhs = gp[p].reshape(2 * blk, gloc)
        for t in range(bands // ntile):
            pacc[0:2 * blk, t * ntile:(t + 1) * ntile] = dot(lhs, wave[t * ntile:(t + 1) * ntile, :], (1, 1))
        live = lax.broadcasted_iota(jnp.int32, (qp, bands), 0) < q
        for r in range(ga):
            off = (r * qa) // apd * blk + (r * qa) % apd * K
            part[stage, r] = jnp.where(live, pacc[off:off + qp, :], 0.0).astype(BF16)
        for d in range(1, ga):
            to = lax.rem(z + d, ga)
            go(remote(part.at[stage, to], prcv.at[stage, d], zs.at[stage, d], zr.at[stage, d], (b, to)))

    def collect(stage, p):
        total = part[stage, z].astype(F32)
        for d in range(1, ga):
            pltpu.make_async_copy(prcv.at[stage, d], prcv.at[stage, d], zr.at[stage, d]).wait()
            total = total + prcv[stage, d].astype(F32)
        where = pl.ds(pl.multiple_of(p * qp, qp), qp)
        cbf[0, where, :] = total.astype(BF16)
        for d in range(1, ga):
            go(remote(cbf.at[0, where], cbf.at[d, where], cs.at[stage, d], cr.at[stage, d],
                      (b, lax.rem(z + d, ga))))

    def got_chip(d, i):
        view = gp.at[from_chip(d), core, :, cols(i)]
        pltpu.make_async_copy(view, view, xr.at[d, i]).wait()

    def got_sib(d, i):
        view = gp.at[from_chip(d), 1 - core, :, cols(i)]
        pltpu.make_async_copy(view, view, sr.at[d, i]).wait()

    def all_sib(d):
        for i in range(PIECES):
            got_sib(d, i)

    all_sib(0)
    project(0, chip)
    if plane:
        for n in range(PIECES):
            i, j = order1[n], order2[n]
            got_chip(1, i)
            if n < half:
                go(chip_copy(3, i, from_chip(1), peer_chip(2), 3))
            go(sib_copy(1, i, from_chip(1)))
            got_chip(2, j)
            if n < half:
                go(chip_copy(3, j, from_chip(2), peer_chip(1), 3))
            go(sib_copy(2, j, from_chip(2)))
        collect(0, chip)
        all_sib(1)
        project(1, from_chip(1))
        all_sib(2)
        project(2, from_chip(2))
        for n in range(half):
            for i in (order1[n], order2[n]):
                got_chip(3, i)
                go(sib_copy(3, i, from_chip(3)))
            if n == 0:
                collect(1, from_chip(1))
        collect(2, from_chip(2))
        all_sib(3)
        project(3, from_chip(3))
        collect(3, from_chip(3))
    else:
        for d in range(1, npair):
            for i in range(PIECES):
                got_chip(d, i)
                go(sib_copy(d, i, from_chip(d)))
            all_sib(d)
            project(d, from_chip(d))
            collect(d - 1, from_chip(d - 1))
        collect(npair - 1, from_chip(npair - 1))

    chi = cbf[0]
    wh, wl = split(chi.astype(F32) * occ_ref[...])
    gram = (dot(chi, wh, (1, 1)) + dot(chi, wl, (1, 1))) * mask[...]
    gh, gl = split(gram)
    dsend[...] = dot(fold[...], gh, (1, 0)) + dot(fold[...], gl, (1, 0))
    for d in range(1, nb):
        go(remote(dsend, drcv.at[d], ds_.at[d], dr.at[d], (lax.rem(b + d, nb), z)))

    arow = lax.broadcasted_iota(jnp.int32, (owned, nspec * 128), 0)
    lane_kind = lax.broadcasted_iota(jnp.int32, (owned, nspec * 128), 1) >> 7
    kind = jnp.zeros((owned, nspec * 128), jnp.int32)
    for j in range(qa):
        for p in range(npair):
            kind = jnp.where(arow == j * npair + p, species_ref[p * unit + z * qa + j], kind)
    onehot = jnp.where(kind == lane_kind, 1.0, 0.0).astype(F32)

    def pick(values):
        values = values * onehot
        return sum(values[:, s * 128:(s + 1) * 128] for s in range(nspec))

    bias_atom = pick(jnp.broadcast_to(bias_pad[0:1, :], onehot.shape))
    out_atom = pick(jnp.broadcast_to(lout_pad[0:1, :], onehot.shape))

    density = dsend[...]
    for d in range(1, nb):
        pltpu.make_async_copy(drcv.at[d], drcv.at[d], dr.at[d]).wait()
        density = density + drcv[d]
    dwide[0:LPAD, :] = density * (1.0 / (bands * nb))
    dts[...] = dwide[...].T
    for k in range(K):
        for j in range(qa):
            dflat[j * npair:(j + 1) * npair, k * LPAD:(k + 1) * LPAD] = \
                dts[pl.ds(j * K + k, npair, stride=qp), :][:, 0:LPAD]
    dh, dl = split(dflat[...])
    pre = pick(dot(dh, whi[...], (1, 0)) + dot(dl, whi[...], (1, 0)) + dot(dh, wlo[...], (1, 0))) + bias_atom
    act = jnp.tanh(pre)
    slopes = out_atom * (1.0 - act * act)
    sh, sl = split(jnp.concatenate([slopes] * nspec, axis=1) * onehot)
    grad = dot(sh, whi[...], (1, 1)) + dot(sl, whi[...], (1, 1)) + dot(sh, wlo[...], (1, 1))
    grad = jnp.concatenate([grad, jnp.zeros((owned, 128), F32)], axis=1)
    for k in range(K):
        for j in range(qa):
            gs[pl.ds(j * K + k, npair, stride=qp), :] = \
                grad[j * npair:(j + 1) * npair, k * LPAD:k * LPAD + 128]
    gh, gl = split(gs[:, 0:LPAD])
    wide = (dot(gh, fold[...], (1, 0)) + dot(gl, fold[...], (1, 0))) * mask[...]
    sym = wide + wide.T
    sh, sl = split(sym)
    scs[...] = dot(fold[...], sh, (1, 0)) + dot(fold[...], sl, (1, 0))
    for d in range(1, ga):
        go(remote(scs, scr.at[d], gs_s.at[d], gs_r.at[d], (b, lax.rem(z + d, ga))))

    factor = 1.0 / jnp.sqrt(F32(nb * apd * K))

    def apply(d, symm):
        sh, sl = split(symm)
        coefs = cbf[d]
        appo[lax.rem(z + ga - d, ga)] = (dot(sh, coefs, (1, 0)) + dot(sl, coefs, (1, 0))) * factor

    apply(0, sym)
    for d in range(1, ga):
        for stage in range(npair):
            where = pl.ds(pl.multiple_of(from_chip(stage) * qp, qp), qp)
            pltpu.make_async_copy(cbf.at[d, where], cbf.at[d, where], cr.at[stage, d]).wait()
        pltpu.make_async_copy(scr.at[d], scr.at[d], gs_r.at[d]).wait()
        sh, sl = split(scr[d])
        apply(d, (dot(fold[...], sh, (0, 0)) + dot(fold[...], sl, (0, 0))) * mask[...])

    for p in range(npair):
        for c in range(2):
            for r in range(c * apd // qa, (c + 1) * apd // qa):
                off = (r * qa) % apd * K
                tmp[off:off + q, :] = appo[r, p * qp:p * qp + q, :]
            app_ref[(p * 2 + c) * blk:(p * 2 + c + 1) * blk, :] = tmp[...].astype(BF16)

    for c in sends:
        c.wait_send()
    for k in keeps:
        k.wait()


def body(wave_coef, projector, occupation, species, layer_in, bias_in, layer_out):
    apd, K, gloc = projector.shape
    nb, ga = lax.axis_size("band"), lax.axis_size("ga")
    bands = wave_coef.shape[0]
    nspec, _, hid = layer_in.shape
    npair = nb // 2
    qa = 2 * apd // ga
    q = qa * K
    qp = 16
    while qp < q:
        qp *= 2
    blk = -(-apd * K // 16) * 16
    rows = npair * qp
    owned = npair * qa
    flat = -(-K * LPAD // 128) * 128
    own = jnp.pad(projector.reshape(apd * K, gloc), ((0, blk - apd * K), (0, 0)))
    vm = pl.BlockSpec(memory_space=pltpu.VMEM)
    hb = pl.BlockSpec(memory_space=pl.ANY)
    sem = pltpu.SemaphoreType.DMA
    app, whole = pl.pallas_call(
        functools.partial(kernel, (nb, ga, apd, K, nspec, hid)),
        out_shape=(
            jax.ShapeDtypeStruct((nb * blk, bands), BF16),
            jax.ShapeDtypeStruct((nb * blk, gloc), BF16),
        ),
        in_specs=[hb, hb, vm, pl.BlockSpec(memory_space=pltpu.SMEM), hb, vm, vm],
        out_specs=(vm, hb),
        scratch_shapes=[
            pltpu.VMEM((npair, 2, blk, gloc), BF16),
            pltpu.VMEM((bands, gloc), BF16),
            pltpu.VMEM((2 * blk + qp, bands), F32),
            pltpu.VMEM((npair, ga, qp, bands), BF16),
            pltpu.VMEM((npair, ga, qp, bands), BF16),
            pltpu.VMEM((ga, rows, bands), BF16),
            pltpu.VMEM(layer_in.shape, F32),
            pltpu.VMEM((flat, nspec * 128), F32),
            pltpu.VMEM((flat, nspec * 128), BF16),
            pltpu.VMEM((flat, nspec * 128), BF16),
            pltpu.VMEM((rows, rows), F32),
            pltpu.VMEM((LPAD, rows), BF16),
            pltpu.VMEM((8, nspec * 128), F32),
            pltpu.VMEM((8, nspec * 128), F32),
            pltpu.VMEM((LPAD, rows), F32),
            pltpu.VMEM((nb, LPAD, rows), F32),
            pltpu.VMEM((128, rows), F32),
            pltpu.VMEM((rows, 128), F32),
            pltpu.VMEM((owned, flat), F32),
            pltpu.VMEM((rows, 128), F32),
            pltpu.VMEM((LPAD, rows), F32),
            pltpu.VMEM((ga, LPAD, rows), F32),
            pltpu.VMEM((ga, rows, bands), F32),
            pltpu.VMEM((blk, bands), F32),
            sem((3,)),
            sem((npair, 2)),
            sem((npair, PIECES)), sem((npair, PIECES)),
            sem((npair, PIECES)), sem((npair, PIECES)),
            sem((npair, ga)), sem((npair, ga)),
            sem((npair, ga)), sem((npair, ga)),
            sem((nb,)), sem((nb,)),
            sem((ga,)), sem((ga,)),
        ],
        compiler_params=pltpu.CompilerParams(collective_id=0, has_side_effects=True,
                                             vmem_limit_bytes=56 * 1024 * 1024),
    )(wave_coef, own, occupation.reshape(1, bands), species, layer_in, bias_in, layer_out)
    corrected = lax.dot_general(app, whole, (((0,), (0,)), ((), ())), preferred_element_type=F32)
    return corrected.astype(BF16)


def solution(mesh):
    in_specs = (P("band", "ga"), P("band", None, "ga"), P("band"), P(), P(), P(), P())
    out_specs = P("band", "ga")
    return jax.shard_map(body, mesh=mesh, in_specs=in_specs, out_specs=out_specs, check_vma=False)
```

```python
import functools

import jax
import jax.numpy as jnp
from jax import lax
from jax.experimental import pallas as pl
from jax.experimental.pallas import tpu as pltpu
from jax.sharding import PartitionSpec as P

MESH = pl.DeviceIdType.MESH
F32 = jnp.float32
BF16 = jnp.bfloat16
PIECES = 4
LPAD = 32


def split(value):
    high = value.astype(BF16)
    return high, (value - high.astype(F32)).astype(BF16)


def dot(a, b, contract):
    return lax.dot_general(a, b, ((contract[:1], contract[1:]), ((), ())), preferred_element_type=F32)


def kernel(dims, wave_hbm, proj_hbm, occ_ref, species_ref, layer_hbm, bias_ref, out_ref,
           app_ref, whole_ref,
           gp, wave, pacc, part, prcv, cbf, layer, wpad, whi, wlo, mask, fold, bias_pad, lout_pad,
           dsend, drcv, dwide, dts, dflat, gs, scs, scr, appo, tmp,
           slot, mine, wide_in, turned, load_sem, keep_sem, xs, xr, ss, sr, zs, zr, cs, cr, ds_, dr, gs_s, gs_r):
    nb, ga, apd, K, nspec, hid = dims
    npair = nb // 2
    unit = 2 * apd
    qa = unit // ga
    q = qa * K
    qp = part.shape[2]
    rows = npair * qp
    blk = gp.shape[2]
    bands, gloc = wave.shape
    owned = npair * qa
    shift = qp.bit_length() - 1
    plane = npair == 4
    b = lax.axis_index("band")
    z = lax.axis_index("ga")
    chip, core = b // 2, b % 2

    def peer_chip(d):
        if plane:
            x, y = chip % 2, chip // 2
            x = 1 - x if d % 2 else x
            y = 1 - y if d // 2 else y
            return y * 2 + x
        return lax.rem(chip + d, npair)

    def from_chip(d):
        if plane:
            return peer_chip(d)
        return lax.rem(chip + npair - d, npair)

    sibling = chip * 2 + 1 - core
    width = gloc // PIECES

    def cols(i):
        return pl.ds(i * width, width)

    loads = [
        pltpu.make_async_copy(proj_hbm, gp.at[chip, core], load_sem.at[0]),
        pltpu.make_async_copy(wave_hbm, wave, load_sem.at[1]),
        pltpu.make_async_copy(layer_hbm, layer, load_sem.at[2]),
    ]
    for c in loads:
        c.start()

    barrier = pltpu.get_barrier_semaphore()
    for d in range(1, nb):
        pl.semaphore_signal(barrier, inc=1, device_id=(lax.rem(b + d, nb), z), device_id_type=MESH)
    for d in range(1, ga):
        pl.semaphore_signal(barrier, inc=1, device_id=(b, lax.rem(z + d, ga)), device_id_type=MESH)
    pl.semaphore_wait(barrier, nb + ga - 2)

    sends = []

    def remote(src, dst, send_sem, recv_sem, where):
        copy = pltpu.make_async_remote_copy(src_ref=src, dst_ref=dst, send_sem=send_sem, recv_sem=recv_sem,
                                            device_id=where, device_id_type=MESH)
        return copy

    def chip_copy(d, i, block_chip, target_chip, send_d):
        view = gp.at[block_chip, core, :, cols(i)]
        return remote(view, view, xs.at[send_d, i], xr.at[d, i], (target_chip * 2 + core, z))

    def sib_copy(d, i, block_chip):
        view = gp.at[block_chip, core, :, cols(i)]
        return remote(view, view, ss.at[d, i], sr.at[d, i], (sibling, z))

    def go(copy):
        copy.start()
        sends.append(copy)

    half = PIECES // 2
    order1 = list(range(PIECES))
    order2 = order1[half:] + order1[:half]
    loads[0].wait()
    for n in range(PIECES):
        if plane:
            go(chip_copy(1, order1[n], chip, peer_chip(1), 1))
            go(chip_copy(2, order2[n], chip, peer_chip(2), 2))
        else:
            for d in range(1, npair):
                go(chip_copy(d, n, chip, peer_chip(d), d))
    for n in range(PIECES):
        go(sib_copy(0, n, chip))

    wpad[...] = jnp.zeros_like(wpad)
    bias_pad[...] = jnp.zeros_like(bias_pad)
    lout_pad[...] = jnp.zeros_like(lout_pad)
    dwide[...] = jnp.zeros_like(dwide)
    gs[...] = jnp.zeros_like(gs)
    dflat[...] = jnp.zeros_like(dflat)
    tmp[...] = jnp.zeros_like(tmp)
    slot[...] = jnp.zeros_like(slot)
    wide_in[...] = jnp.zeros_like(wide_in)

    def place(i, axis_shape, axis):
        idx = lax.broadcasted_iota(jnp.int32, axis_shape, axis)
        pair = idx >> shift
        w = idx - (pair << shift)
        j = jnp.zeros_like(w)
        for t in range(1, qa):
            j = j + (w >= t * K).astype(jnp.int32)
        return pair * qa + j, w - j * K, w < q

    ar, _, vr = place(0, (rows, rows), 0)
    ac, _, vc = place(0, (rows, rows), 1)
    mask[...] = jnp.where((ar == ac) & vr & vc, 1.0, 0.0).astype(F32)
    _, kc, vk = place(0, (LPAD, rows), 1)
    lrow = lax.broadcasted_iota(jnp.int32, (LPAD, rows), 0)
    fold[...] = jnp.where((lrow == kc) & vk, 1.0, 0.0).astype(F32).astype(BF16)

    for s in range(nspec):
        bias_pad[0:1, s * 128:s * 128 + hid] = bias_ref[s:s + 1, :]
        lout_pad[0:1, s * 128:s * 128 + hid] = out_ref[s:s + 1, :]
    loads[2].wait()
    for s in range(nspec):
        wide_in[0:hid, 0:K * K] = layer[:, s, :]
        turned[...] = wide_in[...].T
        for k in range(K):
            wpad[k * LPAD:k * LPAD + K, s * 128:(s + 1) * 128] = turned[k * K:(k + 1) * K, :]
    high, low = split(wpad[...])
    whi[...] = high
    wlo[...] = low
    loads[1].wait()

    keeps = []
    ntile = 256 if bands % 256 == 0 else bands

    def project(stage, p):
        for c in range(2):
            k = pltpu.make_async_copy(gp.at[p, c], whole_ref.at[pl.ds(pl.multiple_of((p * 2 + c) * blk, blk), blk)],
                                      keep_sem.at[stage, c])
            k.start()
            keeps.append(k)
        lhs = gp[p].reshape(2 * blk, gloc)
        for t in range(bands // ntile):
            piece = dot(lhs, wave[t * ntile:(t + 1) * ntile, :], (1, 1))
            for u in range(ntile // 128):
                pacc[t * (ntile // 128) + u] = piece[:, u * 128:(u + 1) * 128]
        own = None
        for r in range(ga):
            for j in range(qa):
                atom = (r * qa + j) % apd
                base = (r * qa + j) // apd * blk + atom
                for u in range(bands // 128):
                    slot[j * K:(j + 1) * K, u * 128:(u + 1) * 128] = pacc[u, pl.ds(base, K, stride=apd), :]
            value = slot[...]
            part[stage, r] = value.astype(BF16)
            own = value if own is None else jnp.where(z == r, value, own)
        mine[stage] = own
        at_end(0, lambda: [push(0, stage, r, 0) for r in range(1, ga)])
        at_end(ga - 1, lambda: [push(1, stage, r, ga - 1) for r in range(ga - 1)])

    line_sends = [[] for _ in range(ga)]

    def at_end(v, work):
        @pl.when(z == v)
        def _():
            work()

    def push(way, stage, r, v):
        to = v + 1 if way == 0 else v - 1

        def make():
            return remote(part.at[stage, r], prcv.at[way, stage, r], zs.at[stage, r], zr.at[way, stage, r], (b, to))
        make().start()
        line_sends[v].append(make)

    def arrive(way, stage, r):
        view = prcv.at[way, stage, r]
        pltpu.make_async_copy(view, view, zr.at[way, stage, r]).wait()
        return prcv[way, stage, r].astype(F32)

    def both_ways(v):
        return (0, 1) if v < ga // 2 else (1, 0)

    def hop(stage):
        def work(v):
            for way in both_ways(v):
                for r in (range(v + 1, ga) if way == 0 else range(v)):
                    part[stage, r] = (part[stage, r].astype(F32) + arrive(way, stage, r)).astype(BF16)
                    push(way, stage, r, v)
        for v in range(1, ga - 1):
            at_end(v, functools.partial(work, v))

    def share(way, p, stage, r, v):
        to = v + 1 if way == 0 else v - 1

        def make():
            view = cbf.at[r, place_of(p)]
            return remote(view, view, cs.at[way, stage, r], cr.at[stage, r], (b, to))
        make().start()
        line_sends[v].append(make)

    def place_of(p):
        return pl.ds(pl.multiple_of(p * qp, qp), qp)

    def collect(stage, p):
        def work(v):
            total = mine[stage]
            if v > 0:
                total = total + arrive(0, stage, v)
            if v < ga - 1:
                total = total + arrive(1, stage, v)
            cbf[v, place_of(p), :] = total.astype(BF16)
            if v > 0:
                share(1, p, stage, v, v)
            if v < ga - 1:
                share(0, p, stage, v, v)
        for v in range(ga):
            at_end(v, functools.partial(work, v))

    def got_share(stage, p, r):
        view = cbf.at[r, place_of(p)]
        pltpu.make_async_copy(view, view, cr.at[stage, r]).wait()

    def spread(stage, p):
        def work(v):
            for way in both_ways(v):
                for r in (range(v - 1, -1, -1) if way == 0 else range(v + 1, ga)):
                    got_share(stage, p, r)
                    if 0 < v < ga - 1:
                        share(way, p, stage, r, v)
        for v in range(ga):
            at_end(v, functools.partial(work, v))

    def got_chip(d, i):
        view = gp.at[from_chip(d), core, :, cols(i)]
        pltpu.make_async_copy(view, view, xr.at[d, i]).wait()

    def got_sib(d, i):
        view = gp.at[from_chip(d), 1 - core, :, cols(i)]
        pltpu.make_async_copy(view, view, sr.at[d, i]).wait()

    def all_sib(d):
        for i in range(PIECES):
            got_sib(d, i)

    all_sib(0)
    project(0, chip)
    if plane:
        for n in range(PIECES):
            i, j = order1[n], order2[n]
            got_chip(1, i)
            if n < half:
                go(chip_copy(3, i, from_chip(1), peer_chip(2), 3))
            go(sib_copy(1, i, from_chip(1)))
            got_chip(2, j)
            if n < half:
                go(chip_copy(3, j, from_chip(2), peer_chip(1), 3))
            go(sib_copy(2, j, from_chip(2)))
            if n == 1:
                hop(0)
            if n == 2:
                collect(0, chip)
        all_sib(1)
        project(1, from_chip(1))
        all_sib(2)
        project(2, from_chip(2))
        spread(0, chip)
        hop(1)
        for n in range(half):
            for i in (order1[n], order2[n]):
                got_chip(3, i)
                go(sib_copy(3, i, from_chip(3)))
            if n == 0:
                hop(2)
                collect(1, from_chip(1))
        collect(2, from_chip(2))
        all_sib(3)
        project(3, from_chip(3))
        spread(1, from_chip(1))
        spread(2, from_chip(2))
        hop(3)
        collect(3, from_chip(3))
    else:
        for d in range(1, npair):
            for i in range(PIECES):
                got_chip(d, i)
                go(sib_copy(d, i, from_chip(d)))
            all_sib(d)
            project(d, from_chip(d))
            hop(d - 1)
            collect(d - 1, from_chip(d - 1))
            spread(d - 1, from_chip(d - 1))
        hop(npair - 1)
        collect(npair - 1, from_chip(npair - 1))

    chi = cbf[z]
    wh, wl = split(chi.astype(F32) * occ_ref[...])
    gram = (dot(chi, wh, (1, 1)) + dot(chi, wl, (1, 1))) * mask[...]
    gh, gl = split(gram)
    dsend[...] = dot(fold[...], gh, (1, 0)) + dot(fold[...], gl, (1, 0))
    for d in range(1, nb):
        go(remote(dsend, drcv.at[d], ds_.at[d], dr.at[d], (lax.rem(b + d, nb), z)))

    arow = lax.broadcasted_iota(jnp.int32, (owned, nspec * 128), 0)
    lane_kind = lax.broadcasted_iota(jnp.int32, (owned, nspec * 128), 1) >> 7
    kind = jnp.zeros((owned, nspec * 128), jnp.int32)
    for j in range(qa):
        for p in range(npair):
            kind = jnp.where(arow == j * npair + p, species_ref[p * unit + z * qa + j], kind)
    onehot = jnp.where(kind == lane_kind, 1.0, 0.0).astype(F32)

    def pick(values):
        values = values * onehot
        return sum(values[:, s * 128:(s + 1) * 128] for s in range(nspec))

    bias_atom = pick(jnp.broadcast_to(bias_pad[0:1, :], onehot.shape))
    out_atom = pick(jnp.broadcast_to(lout_pad[0:1, :], onehot.shape))

    spread(npair - 1, from_chip(npair - 1))
    density = dsend[...]
    for d in range(1, nb):
        pltpu.make_async_copy(drcv.at[d], drcv.at[d], dr.at[d]).wait()
        density = density + drcv[d]
    dwide[0:LPAD, :] = density * (1.0 / (bands * nb))
    dts[...] = dwide[...].T
    for k in range(K):
        for j in range(qa):
            dflat[j * npair:(j + 1) * npair, k * LPAD:(k + 1) * LPAD] = \
                dts[pl.ds(j * K + k, npair, stride=qp), :][:, 0:LPAD]
    dh, dl = split(dflat[...])
    pre = pick(dot(dh, whi[...], (1, 0)) + dot(dl, whi[...], (1, 0)) + dot(dh, wlo[...], (1, 0))) + bias_atom
    act = jnp.tanh(pre)
    slopes = out_atom * (1.0 - act * act)
    sh, sl = split(jnp.concatenate([slopes] * nspec, axis=1) * onehot)
    grad = dot(sh, whi[...], (1, 1)) + dot(sl, whi[...], (1, 1)) + dot(sh, wlo[...], (1, 1))
    grad = jnp.concatenate([grad, jnp.zeros((owned, 128), F32)], axis=1)
    for k in range(K):
        for j in range(qa):
            gs[pl.ds(j * K + k, npair, stride=qp), :] = \
                grad[j * npair:(j + 1) * npair, k * LPAD:k * LPAD + 128]
    gh, gl = split(gs[:, 0:LPAD])
    wide = (dot(gh, fold[...], (1, 0)) + dot(gl, fold[...], (1, 0))) * mask[...]
    sym = wide + wide.T
    sh, sl = split(sym)
    scs[...] = dot(fold[...], sh, (1, 0)) + dot(fold[...], sl, (1, 0))
    for d in range(1, ga):
        go(remote(scs, scr.at[d], gs_s.at[d], gs_r.at[d], (b, lax.rem(z + d, ga))))

    factor = 1.0 / jnp.sqrt(F32(nb * apd * K))

    def apply(d, symm):
        sh, sl = split(symm)
        owner = lax.rem(z + ga - d, ga)
        coefs = cbf[owner]
        appo[owner] = (dot(sh, coefs, (1, 0)) + dot(sl, coefs, (1, 0))) * factor

    apply(0, sym)
    for d in range(1, ga):
        pltpu.make_async_copy(scr.at[d], scr.at[d], gs_r.at[d]).wait()
        sh, sl = split(scr[d])
        apply(d, (dot(fold[...], sh, (0, 0)) + dot(fold[...], sl, (0, 0))) * mask[...])

    for p in range(npair):
        for c in range(2):
            for a in range(apd):
                r, j = (c * apd + a) // qa, (c * apd + a) % qa
                for u in range(bands // 128):
                    tmp[u, pl.ds(a, K, stride=apd), :] = \
                        appo[r, p * qp + j * K:p * qp + (j + 1) * K, u * 128:(u + 1) * 128]
            for u in range(bands // 128):
                app_ref[(p * 2 + c) * blk:(p * 2 + c + 1) * blk, u * 128:(u + 1) * 128] = tmp[u].astype(BF16)

    for c in sends:
        c.wait_send()
    for v in range(ga):
        at_end(v, lambda: [make().wait_send() for make in line_sends[v]])
    for k in keeps:
        k.wait()


def body(wave_coef, projector, occupation, species, layer_in, bias_in, layer_out):
    apd, K, gloc = projector.shape
    nb, ga = lax.axis_size("band"), lax.axis_size("ga")
    bands = wave_coef.shape[0]
    nspec, _, hid = layer_in.shape
    npair = nb // 2
    qa = 2 * apd // ga
    q = qa * K
    qp = 16
    while qp < q:
        qp *= 2
    blk = -(-apd * K // 16) * 16
    rows = npair * qp
    owned = npair * qa
    flat = -(-K * LPAD // 128) * 128
    own = jnp.pad(jnp.swapaxes(projector, 0, 1).reshape(apd * K, gloc), ((0, blk - apd * K), (0, 0)))
    vm = pl.BlockSpec(memory_space=pltpu.VMEM)
    hb = pl.BlockSpec(memory_space=pl.ANY)
    sem = pltpu.SemaphoreType.DMA
    app, whole = pl.pallas_call(
        functools.partial(kernel, (nb, ga, apd, K, nspec, hid)),
        out_shape=(
            jax.ShapeDtypeStruct((nb * blk, bands), BF16),
            jax.ShapeDtypeStruct((nb * blk, gloc), BF16),
        ),
        in_specs=[hb, hb, vm, pl.BlockSpec(memory_space=pltpu.SMEM), hb, vm, vm],
        out_specs=(vm, hb),
        scratch_shapes=[
            pltpu.VMEM((npair, 2, blk, gloc), BF16),
            pltpu.VMEM((bands, gloc), BF16),
            pltpu.VMEM((bands // 128, 2 * blk, 128), F32),
            pltpu.VMEM((npair, ga, qp, bands), BF16),
            pltpu.VMEM((2, npair, ga, qp, bands), BF16),
            pltpu.VMEM((ga, rows, bands), BF16),
            pltpu.VMEM((hid, nspec, K * K), F32),
            pltpu.VMEM((flat, nspec * 128), F32),
            pltpu.VMEM((flat, nspec * 128), BF16),
            pltpu.VMEM((flat, nspec * 128), BF16),
            pltpu.VMEM((rows, rows), F32),
            pltpu.VMEM((LPAD, rows), BF16),
            pltpu.VMEM((8, nspec * 128), F32),
            pltpu.VMEM((8, nspec * 128), F32),
            pltpu.VMEM((LPAD, rows), F32),
            pltpu.VMEM((nb, LPAD, rows), F32),
            pltpu.VMEM((128, rows), F32),
            pltpu.VMEM((rows, 128), F32),
            pltpu.VMEM((owned, flat), F32),
            pltpu.VMEM((rows, 128), F32),
            pltpu.VMEM((LPAD, rows), F32),
            pltpu.VMEM((ga, LPAD, rows), F32),
            pltpu.VMEM((ga, rows, bands), F32),
            pltpu.VMEM((bands // 128, blk, 128), F32),
            pltpu.VMEM((qp, bands), F32),
            pltpu.VMEM((npair, qp, bands), F32),
            pltpu.VMEM((128, -(-K * K // 128) * 128), F32),
            pltpu.VMEM((-(-K * K // 128) * 128, 128), F32),
            sem((3,)),
            sem((npair, 2)),
            sem((npair, PIECES)), sem((npair, PIECES)),
            sem((npair, PIECES)), sem((npair, PIECES)),
            sem((npair, ga)), sem((2, npair, ga)),
            sem((2, npair, ga)), sem((npair, ga)),
            sem((nb,)), sem((nb,)),
            sem((ga,)), sem((ga,)),
        ],
        compiler_params=pltpu.CompilerParams(collective_id=0, has_side_effects=True,
                                             vmem_limit_bytes=56 * 1024 * 1024),
    )(wave_coef, own, occupation.reshape(1, bands), species, jnp.transpose(layer_in, (2, 0, 1)), bias_in, layer_out)
    corrected = lax.dot_general(app, whole, (((0,), (0,)), ((), ())), preferred_element_type=F32)
    return corrected.astype(BF16)


def solution(mesh):
    in_specs = (P("band", "ga"), P("band", None, "ga"), P("band"), P(), P(), P(), P())
    out_specs = P("band", "ga")
    return jax.shard_map(body, mesh=mesh, in_specs=in_specs, out_specs=out_specs, check_vma=False)
```

```python
import functools

import jax
import jax.numpy as jnp
from jax import lax
from jax.experimental import pallas as pl
from jax.experimental.pallas import tpu as pltpu
from jax.sharding import PartitionSpec as P

MESH = pl.DeviceIdType.MESH
F32 = jnp.float32
BF16 = jnp.bfloat16
PIECES = 4
LPAD = 32


def split(value):
    high = value.astype(BF16)
    return high, (value - high.astype(F32)).astype(BF16)


def dot(a, b, contract):
    return lax.dot_general(a, b, ((contract[:1], contract[1:]), ((), ())), preferred_element_type=F32)


def kernel(dims, wave_hbm, proj_hbm, occ_ref, species_ref, layer_hbm, bias_ref, out_ref,
           app_ref, whole_ref,
           gp, wave, pacc, part, prcv, cbf, layer, wpad, whi, wlo, mask, fold, bias_pad, lout_pad,
           dsend, drcv, dwide, dts, dflat, gs, scs, scr, appo, tmp,
           slot, wide_in, turned, load_sem, keep_sem, xs, xr, ss, sr, zs, zr, cs, cr, ds_, dr, gs_s, gs_r):
    nb, ga, apd, K, nspec, hid = dims
    npair = nb // 2
    unit = 2 * apd
    qa = unit // ga
    q = qa * K
    qp = part.shape[2]
    rows = npair * qp
    blk = gp.shape[2]
    bands, gloc = wave.shape
    owned = npair * qa
    shift = qp.bit_length() - 1
    plane = npair == 4
    b = lax.axis_index("band")
    z = lax.axis_index("ga")
    chip, core = b // 2, b % 2

    def peer_chip(d):
        if plane:
            x, y = chip % 2, chip // 2
            x = 1 - x if d % 2 else x
            y = 1 - y if d // 2 else y
            return y * 2 + x
        return lax.rem(chip + d, npair)

    def from_chip(d):
        if plane:
            return peer_chip(d)
        return lax.rem(chip + npair - d, npair)

    sibling = chip * 2 + 1 - core
    width = gloc // PIECES

    def cols(i):
        return pl.ds(i * width, width)

    loads = [
        pltpu.make_async_copy(proj_hbm, gp.at[chip, core], load_sem.at[0]),
        pltpu.make_async_copy(wave_hbm, wave, load_sem.at[1]),
        pltpu.make_async_copy(layer_hbm, layer, load_sem.at[2]),
    ]
    for c in loads:
        c.start()

    barrier = pltpu.get_barrier_semaphore()
    for d in range(1, nb):
        pl.semaphore_signal(barrier, inc=1, device_id=(lax.rem(b + d, nb), z), device_id_type=MESH)
    for d in range(1, ga):
        pl.semaphore_signal(barrier, inc=1, device_id=(b, lax.rem(z + d, ga)), device_id_type=MESH)
    pl.semaphore_wait(barrier, nb + ga - 2)

    sends = []

    def remote(src, dst, send_sem, recv_sem, where):
        copy = pltpu.make_async_remote_copy(src_ref=src, dst_ref=dst, send_sem=send_sem, recv_sem=recv_sem,
                                            device_id=where, device_id_type=MESH)
        return copy

    def chip_copy(d, i, block_chip, target_chip, send_d):
        view = gp.at[block_chip, core, :, cols(i)]
        return remote(view, view, xs.at[send_d, i], xr.at[d, i], (target_chip * 2 + core, z))

    def sib_copy(d, i, block_chip):
        view = gp.at[block_chip, core, :, cols(i)]
        return remote(view, view, ss.at[d, i], sr.at[d, i], (sibling, z))

    def go(copy):
        copy.start()
        sends.append(copy)

    half = PIECES // 2
    order1 = list(range(PIECES))
    order2 = order1[half:] + order1[:half]
    loads[0].wait()
    for n in range(PIECES):
        if plane:
            go(chip_copy(1, order1[n], chip, peer_chip(1), 1))
            go(chip_copy(2, order2[n], chip, peer_chip(2), 2))
        else:
            for d in range(1, npair):
                go(chip_copy(d, n, chip, peer_chip(d), d))
    for n in range(PIECES):
        go(sib_copy(0, n, chip))

    wpad[...] = jnp.zeros_like(wpad)
    bias_pad[...] = jnp.zeros_like(bias_pad)
    lout_pad[...] = jnp.zeros_like(lout_pad)
    dwide[...] = jnp.zeros_like(dwide)
    gs[...] = jnp.zeros_like(gs)
    dflat[...] = jnp.zeros_like(dflat)
    tmp[...] = jnp.zeros_like(tmp)
    slot[...] = jnp.zeros_like(slot)
    wide_in[...] = jnp.zeros_like(wide_in)

    def place(i, axis_shape, axis):
        idx = lax.broadcasted_iota(jnp.int32, axis_shape, axis)
        pair = idx >> shift
        w = idx - (pair << shift)
        j = jnp.zeros_like(w)
        for t in range(1, qa):
            j = j + (w >= t * K).astype(jnp.int32)
        return pair * qa + j, w - j * K, w < q

    ar, _, vr = place(0, (rows, rows), 0)
    ac, _, vc = place(0, (rows, rows), 1)
    mask[...] = jnp.where((ar == ac) & vr & vc, 1.0, 0.0).astype(F32)
    _, kc, vk = place(0, (LPAD, rows), 1)
    lrow = lax.broadcasted_iota(jnp.int32, (LPAD, rows), 0)
    fold[...] = jnp.where((lrow == kc) & vk, 1.0, 0.0).astype(F32).astype(BF16)

    for s in range(nspec):
        bias_pad[0:1, s * 128:s * 128 + hid] = bias_ref[s:s + 1, :]
        lout_pad[0:1, s * 128:s * 128 + hid] = out_ref[s:s + 1, :]
    loads[2].wait()
    for s in range(nspec):
        wide_in[0:hid, 0:K * K] = layer[:, s, :]
        turned[...] = wide_in[...].T
        for k in range(K):
            wpad[k * LPAD:k * LPAD + K, s * 128:(s + 1) * 128] = turned[k * K:(k + 1) * K, :]
    high, low = split(wpad[...])
    whi[...] = high
    wlo[...] = low
    loads[1].wait()

    keeps = []
    ntile = 256 if bands % 256 == 0 else bands

    def project(stage, p):
        for c in range(2):
            k = pltpu.make_async_copy(gp.at[p, c], whole_ref.at[pl.ds(pl.multiple_of((p * 2 + c) * blk, blk), blk)],
                                      keep_sem.at[stage, c])
            k.start()
            keeps.append(k)
        lhs = gp[p].reshape(2 * blk, gloc)
        for t in range(bands // ntile):
            piece = dot(lhs, wave[t * ntile:(t + 1) * ntile, :], (1, 1))
            for u in range(ntile // 128):
                pacc[t * (ntile // 128) + u] = piece[:, u * 128:(u + 1) * 128]
        for r in range(ga):
            for j in range(qa):
                atom = (r * qa + j) % apd
                base = (r * qa + j) // apd * blk + atom
                for u in range(bands // 128):
                    slot[j * K:(j + 1) * K, u * 128:(u + 1) * 128] = pacc[u, pl.ds(base, K, stride=apd), :]
            part[stage, r] = slot[...].astype(BF16)
        for d in range(1, ga):
            to = lax.rem(z + d, ga)
            go(remote(part.at[stage, to], prcv.at[stage, d], zs.at[stage, d], zr.at[stage, d], (b, to)))

    def collect(stage, p):
        total = part[stage, z].astype(F32)
        for d in range(1, ga):
            pltpu.make_async_copy(prcv.at[stage, d], prcv.at[stage, d], zr.at[stage, d]).wait()
            total = total + prcv[stage, d].astype(F32)
        where = pl.ds(pl.multiple_of(p * qp, qp), qp)
        cbf[0, where, :] = total.astype(BF16)
        for d in range(1, ga):
            go(remote(cbf.at[0, where], cbf.at[d, where], cs.at[stage, d], cr.at[stage, d],
                      (b, lax.rem(z + d, ga))))

    def got_chip(d, i):
        view = gp.at[from_chip(d), core, :, cols(i)]
        pltpu.make_async_copy(view, view, xr.at[d, i]).wait()

    def got_sib(d, i):
        view = gp.at[from_chip(d), 1 - core, :, cols(i)]
        pltpu.make_async_copy(view, view, sr.at[d, i]).wait()

    def all_sib(d):
        for i in range(PIECES):
            got_sib(d, i)

    all_sib(0)
    project(0, chip)
    if plane:
        for n in range(PIECES):
            i, j = order1[n], order2[n]
            got_chip(1, i)
            if n < half:
                go(chip_copy(3, i, from_chip(1), peer_chip(2), 3))
            go(sib_copy(1, i, from_chip(1)))
            got_chip(2, j)
            if n < half:
                go(chip_copy(3, j, from_chip(2), peer_chip(1), 3))
            go(sib_copy(2, j, from_chip(2)))
        collect(0, chip)
        all_sib(1)
        project(1, from_chip(1))
        all_sib(2)
        project(2, from_chip(2))
        for n in range(half):
            for i in (order1[n], order2[n]):
                got_chip(3, i)
                go(sib_copy(3, i, from_chip(3)))
        all_sib(3)
        project(3, from_chip(3))
        collect(1, from_chip(1))
        collect(2, from_chip(2))
        collect(3, from_chip(3))
    else:
        for d in range(1, npair):
            for i in range(PIECES):
                got_chip(d, i)
                go(sib_copy(d, i, from_chip(d)))
            all_sib(d)
            project(d, from_chip(d))
            collect(d - 1, from_chip(d - 1))
        collect(npair - 1, from_chip(npair - 1))

    chi = cbf[0]
    wh, wl = split(chi.astype(F32) * occ_ref[...])
    gram = (dot(chi, wh, (1, 1)) + dot(chi, wl, (1, 1))) * mask[...]
    gh, gl = split(gram)
    dsend[...] = dot(fold[...], gh, (1, 0)) + dot(fold[...], gl, (1, 0))
    for d in range(1, nb):
        go(remote(dsend, drcv.at[d], ds_.at[d], dr.at[d], (lax.rem(b + d, nb), z)))

    arow = lax.broadcasted_iota(jnp.int32, (owned, nspec * 128), 0)
    lane_kind = lax.broadcasted_iota(jnp.int32, (owned, nspec * 128), 1) >> 7
    kind = jnp.zeros((owned, nspec * 128), jnp.int32)
    for j in range(qa):
        for p in range(npair):
            kind = jnp.where(arow == j * npair + p, species_ref[p * unit + z * qa + j], kind)
    onehot = jnp.where(kind == lane_kind, 1.0, 0.0).astype(F32)

    def pick(values):
        values = values * onehot
        return sum(values[:, s * 128:(s + 1) * 128] for s in range(nspec))

    bias_atom = pick(jnp.broadcast_to(bias_pad[0:1, :], onehot.shape))
    out_atom = pick(jnp.broadcast_to(lout_pad[0:1, :], onehot.shape))

    density = dsend[...]
    for d in range(1, nb):
        pltpu.make_async_copy(drcv.at[d], drcv.at[d], dr.at[d]).wait()
        density = density + drcv[d]
    dwide[0:LPAD, :] = density * (1.0 / (bands * nb))
    dts[...] = dwide[...].T
    for k in range(K):
        for j in range(qa):
            dflat[j * npair:(j + 1) * npair, k * LPAD:(k + 1) * LPAD] = \
                dts[pl.ds(j * K + k, npair, stride=qp), :][:, 0:LPAD]
    dh, dl = split(dflat[...])
    pre = pick(dot(dh, whi[...], (1, 0)) + dot(dl, whi[...], (1, 0)) + dot(dh, wlo[...], (1, 0))) + bias_atom
    act = jnp.tanh(pre)
    slopes = out_atom * (1.0 - act * act)
    sh, sl = split(jnp.concatenate([slopes] * nspec, axis=1) * onehot)
    grad = dot(sh, whi[...], (1, 1)) + dot(sl, whi[...], (1, 1)) + dot(sh, wlo[...], (1, 1))
    grad = jnp.concatenate([grad, jnp.zeros((owned, 128), F32)], axis=1)
    for k in range(K):
        for j in range(qa):
            gs[pl.ds(j * K + k, npair, stride=qp), :] = \
                grad[j * npair:(j + 1) * npair, k * LPAD:k * LPAD + 128]
    gh, gl = split(gs[:, 0:LPAD])
    wide = (dot(gh, fold[...], (1, 0)) + dot(gl, fold[...], (1, 0))) * mask[...]
    sym = wide + wide.T
    sh, sl = split(sym)
    scs[...] = dot(fold[...], sh, (1, 0)) + dot(fold[...], sl, (1, 0))
    for d in range(1, ga):
        go(remote(scs, scr.at[d], gs_s.at[d], gs_r.at[d], (b, lax.rem(z + d, ga))))

    factor = 1.0 / jnp.sqrt(F32(nb * apd * K))

    def apply(d, symm):
        sh, sl = split(symm)
        coefs = cbf[d]
        appo[lax.rem(z + ga - d, ga)] = (dot(sh, coefs, (1, 0)) + dot(sl, coefs, (1, 0))) * factor

    apply(0, sym)
    for d in range(1, ga):
        for stage in range(npair):
            where = pl.ds(pl.multiple_of(from_chip(stage) * qp, qp), qp)
            pltpu.make_async_copy(cbf.at[d, where], cbf.at[d, where], cr.at[stage, d]).wait()
        pltpu.make_async_copy(scr.at[d], scr.at[d], gs_r.at[d]).wait()
        sh, sl = split(scr[d])
        apply(d, (dot(fold[...], sh, (0, 0)) + dot(fold[...], sl, (0, 0))) * mask[...])

    for p in range(npair):
        for c in range(2):
            for a in range(apd):
                r, j = (c * apd + a) // qa, (c * apd + a) % qa
                for u in range(bands // 128):
                    tmp[u, pl.ds(a, K, stride=apd), :] = \
                        appo[r, p * qp + j * K:p * qp + (j + 1) * K, u * 128:(u + 1) * 128]
            for u in range(bands // 128):
                app_ref[(p * 2 + c) * blk:(p * 2 + c + 1) * blk, u * 128:(u + 1) * 128] = tmp[u].astype(BF16)

    for c in sends:
        c.wait_send()
    for k in keeps:
        k.wait()


def expand(app_ref, whole_ref, out_ref, turned):
    @pl.when(pl.program_id(0) == 0)
    def _():
        turned[...] = app_ref[...].T

    out_ref[...] = dot(turned[...], whole_ref[...], (1, 0)).astype(BF16)


def body(wave_coef, projector, occupation, species, layer_in, bias_in, layer_out):
    apd, K, gloc = projector.shape
    nb, ga = lax.axis_size("band"), lax.axis_size("ga")
    bands = wave_coef.shape[0]
    nspec, _, hid = layer_in.shape
    npair = nb // 2
    qa = 2 * apd // ga
    q = qa * K
    qp = 16
    while qp < q:
        qp *= 2
    blk = -(-apd * K // 16) * 16
    rows = npair * qp
    owned = npair * qa
    flat = -(-K * LPAD // 128) * 128
    own = jnp.pad(jnp.swapaxes(projector, 0, 1).reshape(apd * K, gloc), ((0, blk - apd * K), (0, 0)))
    vm = pl.BlockSpec(memory_space=pltpu.VMEM)
    hb = pl.BlockSpec(memory_space=pl.ANY)
    sem = pltpu.SemaphoreType.DMA
    app, whole = pl.pallas_call(
        functools.partial(kernel, (nb, ga, apd, K, nspec, hid)),
        out_shape=(
            jax.ShapeDtypeStruct((nb * blk, bands), BF16),
            jax.ShapeDtypeStruct((nb * blk, gloc), BF16),
        ),
        in_specs=[hb, hb, vm, pl.BlockSpec(memory_space=pltpu.SMEM), hb, vm, vm],
        out_specs=(vm, hb),
        scratch_shapes=[
            pltpu.VMEM((npair, 2, blk, gloc), BF16),
            pltpu.VMEM((bands, gloc), BF16),
            pltpu.VMEM((bands // 128, 2 * blk, 128), F32),
            pltpu.VMEM((npair, ga, qp, bands), BF16),
            pltpu.VMEM((npair, ga, qp, bands), BF16),
            pltpu.VMEM((ga, rows, bands), BF16),
            pltpu.VMEM((hid, nspec, K * K), F32),
            pltpu.VMEM((flat, nspec * 128), F32),
            pltpu.VMEM((flat, nspec * 128), BF16),
            pltpu.VMEM((flat, nspec * 128), BF16),
            pltpu.VMEM((rows, rows), F32),
            pltpu.VMEM((LPAD, rows), BF16),
            pltpu.VMEM((8, nspec * 128), F32),
            pltpu.VMEM((8, nspec * 128), F32),
            pltpu.VMEM((LPAD, rows), F32),
            pltpu.VMEM((nb, LPAD, rows), F32),
            pltpu.VMEM((128, rows), F32),
            pltpu.VMEM((rows, 128), F32),
            pltpu.VMEM((owned, flat), F32),
            pltpu.VMEM((rows, 128), F32),
            pltpu.VMEM((LPAD, rows), F32),
            pltpu.VMEM((ga, LPAD, rows), F32),
            pltpu.VMEM((ga, rows, bands), F32),
            pltpu.VMEM((bands // 128, blk, 128), F32),
            pltpu.VMEM((qp, bands), F32),
            pltpu.VMEM((128, -(-K * K // 128) * 128), F32),
            pltpu.VMEM((-(-K * K // 128) * 128, 128), F32),
            sem((3,)),
            sem((npair, 2)),
            sem((npair, PIECES)), sem((npair, PIECES)),
            sem((npair, PIECES)), sem((npair, PIECES)),
            sem((npair, ga)), sem((npair, ga)),
            sem((npair, ga)), sem((npair, ga)),
            sem((nb,)), sem((nb,)),
            sem((ga,)), sem((ga,)),
        ],
        compiler_params=pltpu.CompilerParams(collective_id=0, has_side_effects=True,
                                             vmem_limit_bytes=56 * 1024 * 1024),
    )(wave_coef, own, occupation.reshape(1, bands), species, jnp.transpose(layer_in, (2, 0, 1)), bias_in, layer_out)
    tile = 512 if gloc % 512 == 0 else gloc
    return pl.pallas_call(
        expand,
        grid=(gloc // tile,),
        out_shape=jax.ShapeDtypeStruct((bands, gloc), BF16),
        in_specs=[
            pl.BlockSpec((nb * blk, bands), lambda i: (0, 0)),
            pl.BlockSpec((nb * blk, tile), lambda i: (0, i)),
        ],
        out_specs=pl.BlockSpec((bands, tile), lambda i: (0, i)),
        scratch_shapes=[pltpu.VMEM((bands, nb * blk), BF16)],
        compiler_params=pltpu.CompilerParams(vmem_limit_bytes=32 * 1024 * 1024),
    )(app, whole)


def solution(mesh):
    in_specs = (P("band", "ga"), P("band", None, "ga"), P("band"), P(), P(), P(), P())
    out_specs = P("band", "ga")
    return jax.shard_map(body, mesh=mesh, in_specs=in_specs, out_specs=out_specs, check_vma=False)
```
